32 devices in a mesh: row: 8 (over z, x), col: 4 (over y, core).
Axes of the slice: x: 2, y: 2, z: 4, core: 2. Of those that a mesh axis runs over, the one named last changes fastest.
Arguments:
- matrix: float32 [64, 8, 128, 128], P('row', 'col'), may hold values from -0.1875 to 0.1875
- columns: int32 [64, 8], P('row', 'col'), may hold values from 0 to 15
- counts: int32 [64, 4], P('row', 'col'), may hold values from 1 to 2
- fine_guess: float32 [64, 32, 128], P(('col', 'row')), may hold values from -6 to 6
- right_side: float32 [64, 32, 128], P(('row', 'col')), may hold values from -6 to 6
- aggregate: int32 [64], P(('row', 'col')), may hold values from 0 to 7
- restrict: float32 [64, 128, 128], P(('row', 'col')), may hold values from -0.5 to 0.5
Outputs:
- coarse_scaled: float32 [64, 32, 128], P('row')
- residual: float32 [64, 32, 128], P(('row', 'col'))
The draws below stay inside these ranges and needn't reach their ends.
Inputs may be any that keep to these rules, and one draw needn't show every extreme that they name: `counts`: slots at or past the count hold no part of the operator.
All inputs are finite; a program needn't handle non-finite values.
Results may differ from the reference program's by a relative error of at most 0.000071.
Values sent between devices are 32-bit elements; how exact they have to be, the bound alone decides.
A program may use at most 64 MiB of HBM per device.

```python
import jax
import jax.numpy as jnp
from jax import lax

BS = 128
CW = 128
KB = 2
NC_GRP = 8
BR_DEV = 2
NV = 32
GR = 8
CG = 16
NB = 64
N_ROW = 8
N_COL = 4


def place_ends(values, own_key, low, high):
    dims = values.shape
    index_at = [jax.random.randint(jax.random.fold_in(own_key, axis), (), 0, dims[axis]) for axis in range(len(dims))]
    values = values.at[tuple(index_at)].set(low)
    longest = dims.index(max(dims))
    index_at[longest] = (index_at[longest] + 1) % dims[longest]
    return values.at[tuple(index_at)].set(high)


def block_levels(key, shape, shards, low, top_value):
    def one(dim, parts):
        draws = jax.random.uniform(jax.random.fold_in(jax.random.fold_in(key, 6), dim), (parts,), jnp.float32, low / len(shards), top_value / len(shards))
        return jnp.repeat(jnp.exp(draws), shape[dim] // parts).reshape((-1,) + (1,) * (len(shape) - dim - 1))

    factor_of = one(*shards[0])
    for cut in shards[1:]:
        factor_of = factor_of * one(*cut)
    return factor_of


def centred(rng, extent, width, limit, split=(), kind=jnp.bfloat16):
    array = jax.random.normal(rng, extent, jnp.float32) * width
    if len(split) > 0:
        array = block_levels(rng, extent, split, -0.22, 0.18) * array
    return jnp.clip(array, min=-limit, max=limit).astype(kind)


def setup_inputs(seed: int = 0) -> dict:
    keys = jax.random.split(jax.random.key(seed), 8)
    matrix = centred(keys[0], (NB, N_COL * KB, BS, BS), (BS * KB * N_COL) ** -0.5, 0.1875, ((0, 8), (1, 4)), jnp.float32)
    columns = place_ends(jax.random.randint(keys[1], (NB, N_COL * KB), 0, BR_DEV * N_ROW), jax.random.fold_in(keys[1], 1), 0, (BR_DEV * N_ROW) - 1).astype(jnp.int32)
    counts = place_ends(jax.random.randint(keys[2], (NB, N_COL), 1, KB + 1), jax.random.fold_in(keys[2], 1), 1, KB).astype(jnp.int32)
    fine_guess = centred(keys[3], (NB, NV, BS), 1.0, 6.0, ((0, 32),), jnp.float32)
    right_side = centred(keys[4], (NB, NV, BS), 1.0, 6.0, ((0, 32),), jnp.float32)
    aggregate = place_ends(jax.random.randint(keys[5], (NB,), 0, NC_GRP), jax.random.fold_in(keys[5], 1), 0, NC_GRP - 1).astype(jnp.int32)
    restrict = centred(keys[6], (NB, BS, CW), BS ** -0.5, 0.5, ((0, 32),), jnp.float32)
    return dict(matrix=matrix, columns=columns, counts=counts, fine_guess=fine_guess, right_side=right_side, aggregate=aggregate, restrict=restrict)


def reference(matrix, columns, counts, fine_guess, right_side, aggregate, restrict):
    slot_total = N_COL * KB
    slot_index = jnp.arange(slot_total, dtype=jnp.int32)
    slot_group = slot_index // KB
    global_col = (slot_group[None, :] * CG + columns).astype(jnp.int32)
    usable = (slot_index % KB)[None, :] < counts[:, slot_group]
    picked = fine_guess[global_col] * usable[:, :, None, None].astype(jnp.float32)
    product = jnp.einsum('gsab,gsvb->gva', matrix, picked, precision=lax.Precision.HIGHEST)
    residual = right_side - product
    mean_sq = lax.optimization_barrier(jnp.mean(residual * residual, axis=(0, 2)))
    scale_rms = jnp.sqrt(mean_sq + 1e-06)
    contrib = jnp.einsum('gva,gak->gvk', residual, restrict, precision=lax.Precision.HIGHEST)
    target = (jnp.arange(NB, dtype=jnp.int32) // GR * NC_GRP + aggregate).astype(jnp.int32)
    coarse = jax.ops.segment_sum(contrib, target, num_segments=NC_GRP * N_ROW)
    return (coarse / scale_rms[None, :, None], residual)
```

```python
import functools

import jax
import jax.numpy as jnp
from jax import lax
from jax.experimental import pallas as pl
from jax.experimental.pallas import tpu as pltpu
from jax.sharding import PartitionSpec as P

NC_GRP = 8
F32 = jnp.float32
BF16 = jnp.bfloat16


def offsets(count):
    inner = 2 if count % 2 == 0 else 1
    outer = count // inner
    steps = [(o, i) for o in range(outer) for i in range(inner) if (o, i) != (0, 0)]
    steps.sort(key=lambda s: -min(s[0], outer - s[0]))
    return inner, outer, steps


def peer(index, inner, outer, step):
    high = lax.rem(lax.div(index, inner) + step[0], outer)
    low = lax.rem(lax.rem(index, inner) + step[1], inner)
    return high * inner + low


def split(value):
    high = value.astype(BF16)
    return high, (value - high.astype(F32)).astype(BF16)


def dot4(left, right):
    m, n = left.shape[0], right.shape[1] // 2
    both = jnp.concatenate(split(left), axis=0)
    out = jnp.dot(both, right, preferred_element_type=F32)
    return out[:m, :n] + (out[:m, n:] + out[m:, :n]) + out[m:, n:]


def kernel(
    n_row, n_col, columns, counts, aggregate, matrix, guess, right_side, restrict,
    coarse_out, residual_out,
    xbuf, mbuf, wbuf, rbuf, rwbuf, rhs, part, part_in, agg_own, agg_in, con, con_in, sq, sq_in,
    load_sem, mat_sem, zsend, zrecv, xsend, xrecv, psend, precv, asend, arecv, csend, crecv, qsend, qrecv,
):
    row, col = lax.axis_index("row"), lax.axis_index("col")
    n_dev = n_row * n_col
    me = row * n_col + col
    blocks = guess.shape[0]
    own_rows = right_side.shape[0]
    slots = matrix.shape[1]
    nv = guess.shape[1]
    width = matrix.shape[3]
    r_in, r_out, _ = offsets(n_row)
    c_in, c_out, c_steps = offsets(n_col)
    z_steps = sorted(range(1, r_out), key=lambda s: -min(s, r_out - s))
    z_wait = sorted(range(1, r_out), key=lambda s: min(s, r_out - s))
    c_peers = [peer(col, c_in, c_out, s) for s in c_steps]
    z_peers = {s: peer(row, r_in, r_out, (s, 0)) for s in z_steps}
    x_steps = list(range(1, r_in))
    x_peers = {s: peer(row, r_in, r_out, (0, s)) for s in x_steps}

    own_slot = pl.ds(row * blocks, blocks)
    load_guess = pltpu.make_async_copy(guess, xbuf.at[own_slot], load_sem.at[0])
    load_guess.start()
    barrier = pltpu.get_barrier_semaphore()
    for p in list(z_peers.values()) + list(x_peers.values()):
        pl.semaphore_signal(barrier, inc=1, device_id=(p, col), device_id_type=pl.DeviceIdType.MESH)
    for p in c_peers:
        pl.semaphore_signal(barrier, inc=1, device_id=(row, p), device_id_type=pl.DeviceIdType.MESH)
    mat_loads = [pltpu.make_async_copy(matrix.at[g], mbuf.at[g], mat_sem.at[g]) for g in range(matrix.shape[0])]
    for c in mat_loads:
        c.start()
    load_restrict = pltpu.make_async_copy(restrict, rbuf, load_sem.at[1])
    load_restrict.start()
    load_rhs = pltpu.make_async_copy(right_side, rhs, load_sem.at[2])
    load_rhs.start()
    for i in range(own_rows):
        agg_own[i] = jnp.full((8, 128), aggregate[i], jnp.int32).astype(F32)
    load_guess.wait()
    pl.semaphore_wait(barrier, len(z_peers) + len(x_peers) + len(c_peers))

    def remote(src, dst, ssem, rsem, r, c):
        return pltpu.make_async_remote_copy(
            src_ref=src, dst_ref=dst, send_sem=ssem, recv_sem=rsem,
            device_id=(r, c), device_id_type=pl.DeviceIdType.MESH,
        )

    sends = []
    z_copies = {}
    for s in z_steps:
        z_copies[s] = remote(xbuf.at[own_slot], xbuf.at[own_slot], zsend.at[s], zrecv.at[s], z_peers[s], col)
        z_copies[s].start()
    x_copies = []
    for s in x_steps:
        c = remote(xbuf.at[own_slot], xbuf.at[own_slot], xsend.at[s, 0], xrecv.at[s, 0], x_peers[s], col)
        c.start()
        x_copies.append(c)
    a_copies = []
    for k, p in enumerate(c_peers):
        c = remote(agg_own, agg_in.at[k], asend.at[k], arecv.at[k], row, p)
        c.start()
        a_copies.append(c)

    for g in range(matrix.shape[0]):
        mat_loads[g].wait()
        for s in range(slots):
            high, low = split(mbuf[g, s].T)
            wbuf[g, s * width:(s + 1) * width, :width] = high
            wbuf[g, s * width:(s + 1) * width, width:] = low
    load_restrict.wait()
    for i in range(own_rows):
        high, low = split(rbuf[i])
        rwbuf[i, :, :high.shape[1]] = high
        rwbuf[i, :, high.shape[1]:] = low

    for s in z_wait:
        z_copies[s].wait_recv()
        source = peer(row, r_in, r_out, (r_out - s, 0))
        got = pl.ds(source * blocks, blocks)
        for t in x_steps:
            c = remote(xbuf.at[got], xbuf.at[got], xsend.at[t, s], xrecv.at[t, s], x_peers[t], col)
            c.start()
            x_copies.append(c)
    for c in x_copies:
        c.wait_recv()

    def product(g):
        picked = []
        for s in range(slots):
            use = jnp.where(s < counts[0, g], 1.0, 0.0).astype(F32)
            picked.append(xbuf[columns[s, g]] * use)
        return dot4(jnp.concatenate(picked, axis=1), wbuf[g])

    p_copies = []
    for k, p in enumerate(c_peers):
        for i in range(own_rows):
            part[k, i] = product(p * own_rows + i)
        c = remote(part.at[k], part_in.at[k], psend.at[k], precv.at[k], row, p)
        c.start()
        p_copies.append(c)
    load_rhs.wait()
    res = [rhs[i] - product(col * own_rows + i) for i in range(own_rows)]
    for k in reversed(range(len(c_peers))):
        p_copies[k].wait_recv()
        for i in range(own_rows):
            res[i] = res[i] - part_in[k, i]

    squares = res[0] * res[0]
    for i in range(1, own_rows):
        squares = squares + res[i] * res[i]
    eye = lax.broadcasted_iota(jnp.int32, (nv, 128), 0) == lax.broadcasted_iota(jnp.int32, (nv, 128), 1)
    by_v = jnp.sum(squares, axis=1, keepdims=True)
    own_sq = jnp.sum(jnp.where(eye, by_v, 0.0), axis=0, keepdims=True)
    sq[...] = own_sq

    def send_squares(d, carry):
        t = lax.rem(me + d, n_dev)
        remote(sq, sq_in.at[d - 1], qsend, qrecv, lax.div(t, n_col), lax.rem(t, n_col)).start()
        return carry

    lax.fori_loop(1, n_dev, send_squares, 0)

    contrib = []
    for i in range(own_rows):
        contrib.append(dot4(res[i], rwbuf[i]))
        con[i] = contrib[i]
    c_copies = []
    for k, p in enumerate(c_peers):
        c = remote(con, con_in.at[k], csend.at[k], crecv.at[k], row, p)
        c.start()
        c_copies.append(c)
    for i in range(own_rows):
        residual_out[i] = res[i]

    def spread(ids, value, total):
        shaped = value.reshape(nv // 8, 8, value.shape[1])
        return [t + jnp.where(ids == c, 1.0, 0.0)[None] * shaped for c, t in enumerate(total)]

    for i in range(own_rows):
        for c in range(NC_GRP):
            mask = jnp.where(agg_own[i] == c, 1.0, 0.0)[None]
            term = mask * contrib[i].reshape(nv // 8, 8, 128)
            if i == 0:
                coarse_out[c] = term.reshape(nv, 128)
            else:
                coarse_out[c] += term.reshape(nv, 128)
    for c in a_copies:
        c.wait_recv()
    for c in c_copies:
        c.wait_recv()
    for c in range(NC_GRP):
        total = coarse_out[c].reshape(nv // 8, 8, 128)
        for k in range(len(c_peers)):
            for i in range(own_rows):
                mask = jnp.where(agg_in[k, i] == c, 1.0, 0.0)[None]
                total = total + mask * con_in[k, i].reshape(nv // 8, 8, 128)
        coarse_out[c] = total.reshape(nv, 128)

    pltpu.make_async_copy(sq_in, sq_in, qrecv).wait()
    all_sq = own_sq + jnp.sum(sq_in[...], axis=0)
    total_v = jnp.sum(jnp.where(eye, all_sq, 0.0), axis=1, keepdims=True)
    inv = 1.0 / jnp.sqrt(total_v / (n_dev * own_rows * 128) + 1e-06)
    for c in range(NC_GRP):
        coarse_out[c] = coarse_out[c] * inv

    for c in list(z_copies.values()) + x_copies + a_copies + p_copies + c_copies:
        c.wait_send()
    pltpu.make_async_copy(sq_in, sq_in, qsend).wait()


def local(n_row, n_col, matrix, columns, counts, fine_guess, right_side, aggregate, restrict):
    blocks, nv, bs = fine_guess.shape
    rows, slots = matrix.shape[:2]
    own_rows = right_side.shape[0]
    cw = restrict.shape[2]
    nc1 = n_col - 1
    r_in, r_out, _ = offsets(n_row)
    dma = pltpu.SemaphoreType.DMA
    vmem = pl.BlockSpec(memory_space=pltpu.VMEM)
    smem = pl.BlockSpec(memory_space=pltpu.SMEM)
    hbm = pl.BlockSpec(memory_space=pl.ANY)
    return pl.pallas_call(
        functools.partial(kernel, n_row, n_col),
        out_shape=(
            jax.ShapeDtypeStruct((NC_GRP, nv, cw), F32),
            jax.ShapeDtypeStruct(right_side.shape, F32),
        ),
        in_specs=[smem] * 3 + [hbm] * 4,
        out_specs=(vmem, vmem),
        scratch_shapes=[
            pltpu.VMEM((n_row * blocks, nv, bs), F32),
            pltpu.VMEM(matrix.shape, F32),
            pltpu.VMEM((rows, slots * bs, 2 * bs), BF16),
            pltpu.VMEM(restrict.shape, F32),
            pltpu.VMEM((own_rows, bs, 2 * cw), BF16),
            pltpu.VMEM(right_side.shape, F32),
            pltpu.VMEM((nc1, own_rows, nv, bs), F32),
            pltpu.VMEM((nc1, own_rows, nv, bs), F32),
            pltpu.VMEM((own_rows, 8, 128), F32),
            pltpu.VMEM((nc1, own_rows, 8, 128), F32),
            pltpu.VMEM((own_rows, nv, cw), F32),
            pltpu.VMEM((nc1, own_rows, nv, cw), F32),
            pltpu.VMEM((1, 128), F32),
            pltpu.VMEM((n_row * n_col - 1, 1, 128), F32),
            dma((3,)), dma((rows,)),
            dma((r_out,)), dma((r_out,)),
            dma((max(r_in, 2), r_out)), dma((max(r_in, 2), r_out)),
            dma((nc1,)), dma((nc1,)),
            dma((nc1,)), dma((nc1,)),
            dma((nc1,)), dma((nc1,)),
            dma(()), dma(()),
        ],
        compiler_params=pltpu.CompilerParams(collective_id=0, has_side_effects=True),
        name="residual_restrict",
    )(columns.T, counts.T, aggregate, matrix, fine_guess, right_side, restrict)


def solution(mesh):
    in_specs = (
        P("row", "col", None, None),
        P("row", "col"),
        P("row", "col"),
        P(("col", "row"), None, None),
        P(("row", "col"), None, None),
        P(("row", "col")),
        P(("row", "col"), None, None),
    )
    out_specs = (P("row", None, None), P(("row", "col"), None, None))
    body = functools.partial(local, mesh.shape["row"], mesh.shape["col"])
    return jax.shard_map(body, mesh=mesh, in_specs=in_specs, out_specs=out_specs, check_vma=False)
```

```python
import functools

import jax
import jax.numpy as jnp
from jax import lax
from jax.experimental import pallas as pl
from jax.experimental.pallas import tpu as pltpu
from jax.sharding import PartitionSpec as P

NC_GRP = 8
F32 = jnp.float32
BF16 = jnp.bfloat16


def offsets(count):
    inner = 2 if count % 2 == 0 else 1
    outer = count // inner
    steps = [(o, i) for o in range(outer) for i in range(inner) if (o, i) != (0, 0)]
    steps.sort(key=lambda s: -min(s[0], outer - s[0]))
    return inner, outer, steps


def peer(index, inner, outer, step):
    high = lax.rem(lax.div(index, inner) + step[0], outer)
    low = lax.rem(lax.rem(index, inner) + step[1], inner)
    return high * inner + low


def split(value):
    high = value.astype(BF16)
    return high, (value - high.astype(F32)).astype(BF16)


def dot4(left, right):
    m, n = left.shape[0], right.shape[1] // 2
    both = jnp.concatenate(split(left), axis=0)
    out = jnp.dot(both, right, preferred_element_type=F32)
    return out[:m, :n] + (out[:m, n:] + out[m:, :n]) + out[m:, n:]


def kernel(
    n_row, n_col, columns_hbm, counts_hbm, aggregate_hbm, matrix, guess, right_side, restrict,
    coarse_out, residual_out,
    columns, counts, aggregate, xbuf, mbuf, wbuf, rbuf, rwbuf, rhs, part, part_in, agg_own, agg_in, con, con_in, sq, sq_in,
    load_sem, mat_sem, zsend, zrecv, xsend, xrecv, psend, precv, asend, arecv, csend, crecv, qsend, qrecv,
):
    row, col = lax.axis_index("row"), lax.axis_index("col")
    n_dev = n_row * n_col
    me = row * n_col + col
    blocks = guess.shape[0]
    own_rows = right_side.shape[0]
    slots = matrix.shape[1]
    nv = guess.shape[1]
    width = matrix.shape[3]
    r_in, r_out, _ = offsets(n_row)
    c_in, c_out, c_steps = offsets(n_col)
    z_steps = sorted(range(1, r_out), key=lambda s: -min(s, r_out - s))
    z_wait = sorted(range(1, r_out), key=lambda s: min(s, r_out - s))
    c_peers = [peer(col, c_in, c_out, s) for s in c_steps]
    z_peers = {s: peer(row, r_in, r_out, (s, 0)) for s in z_steps}
    x_steps = list(range(1, r_in))
    x_peers = {s: peer(row, r_in, r_out, (0, s)) for s in x_steps}

    own_slot = pl.ds(row * blocks, blocks)
    load_guess = pltpu.make_async_copy(guess, xbuf.at[own_slot], load_sem.at[0])
    load_guess.start()
    scalars = ((columns_hbm, columns), (counts_hbm, counts), (aggregate_hbm, aggregate))
    scalar_loads = [pltpu.make_async_copy(a, b, load_sem.at[3 + i]) for i, (a, b) in enumerate(scalars)]
    barrier = pltpu.get_barrier_semaphore()
    for p in list(z_peers.values()) + list(x_peers.values()):
        pl.semaphore_signal(barrier, inc=1, device_id=(p, col), device_id_type=pl.DeviceIdType.MESH)
    for p in c_peers:
        pl.semaphore_signal(barrier, inc=1, device_id=(row, p), device_id_type=pl.DeviceIdType.MESH)
    for c in reversed(scalar_loads):
        c.start()
    mat_loads = [pltpu.make_async_copy(matrix.at[g], mbuf.at[g], mat_sem.at[g]) for g in range(matrix.shape[0])]
    for c in mat_loads:
        c.start()
    load_restrict = pltpu.make_async_copy(restrict, rbuf, load_sem.at[1])
    load_restrict.start()
    load_rhs = pltpu.make_async_copy(right_side, rhs, load_sem.at[2])
    load_rhs.start()
    load_guess.wait()
    pl.semaphore_wait(barrier, len(z_peers) + len(x_peers) + len(c_peers))

    def remote(src, dst, ssem, rsem, r, c):
        return pltpu.make_async_remote_copy(
            src_ref=src, dst_ref=dst, send_sem=ssem, recv_sem=rsem,
            device_id=(r, c), device_id_type=pl.DeviceIdType.MESH,
        )

    sends = []
    z_copies = {}
    for s in z_steps:
        z_copies[s] = remote(xbuf.at[own_slot], xbuf.at[own_slot], zsend.at[s], zrecv.at[s], z_peers[s], col)
        z_copies[s].start()
    x_copies = []
    for s in x_steps:
        c = remote(xbuf.at[own_slot], xbuf.at[own_slot], xsend.at[s, 0], xrecv.at[s, 0], x_peers[s], col)
        c.start()
        x_copies.append(c)
    scalar_loads[2].wait()
    for i in range(own_rows):
        agg_own[i] = jnp.full((8, 128), aggregate[i], jnp.int32).astype(F32)
    a_copies = []
    for k, p in enumerate(c_peers):
        c = remote(agg_own, agg_in.at[k], asend.at[k], arecv.at[k], row, p)
        c.start()
        a_copies.append(c)

    for g in range(matrix.shape[0]):
        mat_loads[g].wait()
        for s in range(slots):
            high, low = split(mbuf[g, s].T)
            wbuf[g, s * width:(s + 1) * width, :width] = high
            wbuf[g, s * width:(s + 1) * width, width:] = low
    load_restrict.wait()
    for i in range(own_rows):
        high, low = split(rbuf[i])
        rwbuf[i, :, :high.shape[1]] = high
        rwbuf[i, :, high.shape[1]:] = low

    for s in z_wait:
        z_copies[s].wait_recv()
        source = peer(row, r_in, r_out, (r_out - s, 0))
        got = pl.ds(source * blocks, blocks)
        for t in x_steps:
            c = remote(xbuf.at[got], xbuf.at[got], xsend.at[t, s], xrecv.at[t, s], x_peers[t], col)
            c.start()
            x_copies.append(c)
    for c in x_copies:
        c.wait_recv()

    scalar_loads[0].wait()
    scalar_loads[1].wait()

    def product(g):
        picked = []
        for s in range(slots):
            use = jnp.where(s < counts[0, g], 1.0, 0.0).astype(F32)
            picked.append(xbuf[columns[s, g]] * use)
        return dot4(jnp.concatenate(picked, axis=1), wbuf[g])

    p_copies = []
    for k, p in enumerate(c_peers):
        for i in range(own_rows):
            part[k, i] = product(p * own_rows + i)
        c = remote(part.at[k], part_in.at[k], psend.at[k], precv.at[k], row, p)
        c.start()
        p_copies.append(c)
    load_rhs.wait()
    res = [rhs[i] - product(col * own_rows + i) for i in range(own_rows)]
    for k in reversed(range(len(c_peers))):
        p_copies[k].wait_recv()
        for i in range(own_rows):
            res[i] = res[i] - part_in[k, i]

    squares = res[0] * res[0]
    for i in range(1, own_rows):
        squares = squares + res[i] * res[i]
    eye = lax.broadcasted_iota(jnp.int32, (nv, 128), 0) == lax.broadcasted_iota(jnp.int32, (nv, 128), 1)
    by_v = jnp.sum(squares, axis=1, keepdims=True)
    own_sq = jnp.sum(jnp.where(eye, by_v, 0.0), axis=0, keepdims=True)
    sq[...] = own_sq

    def send_squares(d, carry):
        t = lax.rem(me + d, n_dev)
        remote(sq, sq_in.at[d - 1], qsend, qrecv, lax.div(t, n_col), lax.rem(t, n_col)).start()
        return carry

    lax.fori_loop(1, n_dev, send_squares, 0)

    contrib = []
    for i in range(own_rows):
        contrib.append(dot4(res[i], rwbuf[i]))
        con[i] = contrib[i]
    c_copies = []
    for k, p in enumerate(c_peers):
        c = remote(con, con_in.at[k], csend.at[k], crecv.at[k], row, p)
        c.start()
        c_copies.append(c)
    for i in range(own_rows):
        residual_out[i] = res[i]

    def spread(ids, value, total):
        shaped = value.reshape(nv // 8, 8, value.shape[1])
        return [t + jnp.where(ids == c, 1.0, 0.0)[None] * shaped for c, t in enumerate(total)]

    for i in range(own_rows):
        for c in range(NC_GRP):
            mask = jnp.where(agg_own[i] == c, 1.0, 0.0)[None]
            term = mask * contrib[i].reshape(nv // 8, 8, 128)
            if i == 0:
                coarse_out[c] = term.reshape(nv, 128)
            else:
                coarse_out[c] += term.reshape(nv, 128)
    for c in a_copies:
        c.wait_recv()
    for c in c_copies:
        c.wait_recv()
    for c in range(NC_GRP):
        total = coarse_out[c].reshape(nv // 8, 8, 128)
        for k in range(len(c_peers)):
            for i in range(own_rows):
                mask = jnp.where(agg_in[k, i] == c, 1.0, 0.0)[None]
                total = total + mask * con_in[k, i].reshape(nv // 8, 8, 128)
        coarse_out[c] = total.reshape(nv, 128)

    pltpu.make_async_copy(sq_in, sq_in, qrecv).wait()
    all_sq = own_sq + jnp.sum(sq_in[...], axis=0)
    total_v = jnp.sum(jnp.where(eye, all_sq, 0.0), axis=1, keepdims=True)
    inv = 1.0 / jnp.sqrt(total_v / (n_dev * own_rows * 128) + 1e-06)
    for c in range(NC_GRP):
        coarse_out[c] = coarse_out[c] * inv

    for c in list(z_copies.values()) + x_copies + a_copies + p_copies + c_copies:
        c.wait_send()
    pltpu.make_async_copy(sq_in, sq_in, qsend).wait()


def local(n_row, n_col, matrix, columns, counts, fine_guess, right_side, aggregate, restrict):
    blocks, nv, bs = fine_guess.shape
    rows, slots = matrix.shape[:2]
    own_rows = right_side.shape[0]
    cw = restrict.shape[2]
    nc1 = n_col - 1
    r_in, r_out, _ = offsets(n_row)
    dma = pltpu.SemaphoreType.DMA
    vmem = pl.BlockSpec(memory_space=pltpu.VMEM)
    hbm = pl.BlockSpec(memory_space=pl.ANY)
    return pl.pallas_call(
        functools.partial(kernel, n_row, n_col),
        out_shape=(
            pltpu.VMEM((NC_GRP, nv, cw), F32),
            pltpu.VMEM(right_side.shape, F32),
        ),
        in_specs=[hbm] * 7,
        out_specs=(vmem, vmem),
        scratch_shapes=[
            pltpu.SMEM((slots, rows), jnp.int32),
            pltpu.SMEM((1, rows), jnp.int32),
            pltpu.SMEM((own_rows,), jnp.int32),
            pltpu.VMEM((n_row * blocks, nv, bs), F32),
            pltpu.VMEM(matrix.shape, F32),
            pltpu.VMEM((rows, slots * bs, 2 * bs), BF16),
            pltpu.VMEM(restrict.shape, F32),
            pltpu.VMEM((own_rows, bs, 2 * cw), BF16),
            pltpu.VMEM(right_side.shape, F32),
            pltpu.VMEM((nc1, own_rows, nv, bs), F32),
            pltpu.VMEM((nc1, own_rows, nv, bs), F32),
            pltpu.VMEM((own_rows, 8, 128), F32),
            pltpu.VMEM((nc1, own_rows, 8, 128), F32),
            pltpu.VMEM((own_rows, nv, cw), F32),
            pltpu.VMEM((nc1, own_rows, nv, cw), F32),
            pltpu.VMEM((1, 128), F32),
            pltpu.VMEM((n_row * n_col - 1, 1, 128), F32),
            dma((6,)), dma((rows,)),
            dma((r_out,)), dma((r_out,)),
            dma((max(r_in, 2), r_out)), dma((max(r_in, 2), r_out)),
            dma((nc1,)), dma((nc1,)),
            dma((nc1,)), dma((nc1,)),
            dma((nc1,)), dma((nc1,)),
            dma(()), dma(()),
        ],
        compiler_params=pltpu.CompilerParams(collective_id=0, has_side_effects=True),
        name="residual_restrict",
    )(columns.T, counts.T, aggregate, matrix, fine_guess, right_side, restrict)


def solution(mesh):
    in_specs = (
        P("row", "col", None, None),
        P("row", "col"),
        P("row", "col"),
        P(("col", "row"), None, None),
        P(("row", "col"), None, None),
        P(("row", "col")),
        P(("row", "col"), None, None),
    )
    out_specs = (P("row", None, None), P(("row", "col"), None, None))
    body = functools.partial(local, mesh.shape["row"], mesh.shape["col"])
    return jax.shard_map(body, mesh=mesh, in_specs=in_specs, out_specs=out_specs, check_vma=False)
```

```python
import functools

import jax
import jax.numpy as jnp
from jax import lax
from jax.experimental import pallas as pl
from jax.experimental.pallas import tpu as pltpu
from jax.sharding import PartitionSpec as P

NC_GRP = 8
F32 = jnp.float32
BF16 = jnp.bfloat16


def offsets(count):
    inner = 2 if count % 2 == 0 else 1
    outer = count // inner
    steps = [(o, i) for o in range(outer) for i in range(inner) if (o, i) != (0, 0)]
    steps.sort(key=lambda s: -min(s[0], outer - s[0]))
    return inner, outer, steps


def peer(index, inner, outer, step):
    high = lax.rem(lax.div(index, inner) + step[0], outer)
    low = lax.rem(lax.rem(index, inner) + step[1], inner)
    return high * inner + low


def swap(index, step, count):
    out, bit = 0, 1
    while bit < count:
        out = out + lax.rem(lax.div(index, bit) + (step // bit) % 2, 2) * bit
        bit *= 2
    return out


def row_peer(row, inner, outer, step, back=False):
    low = lax.rem(lax.rem(row, inner) + step[1], inner)
    if outer & (outer - 1):
        high = lax.rem(lax.div(row, inner) + (outer - step[0] if back else step[0]), outer)
    else:
        high = swap(lax.div(row, inner), step[0], outer)
    return high * inner + low


def split(value):
    high = value.astype(BF16)
    return high, (value - high.astype(F32)).astype(BF16)


def dot4(left, right):
    m, n = left.shape[0], right.shape[1] // 2
    both = jnp.concatenate(split(left), axis=0)
    out = jnp.dot(both, right, preferred_element_type=F32)
    return out[:m, :n] + (out[:m, n:] + out[m:, :n]) + out[m:, n:]


def kernel(
    n_row, n_col, columns_hbm, counts_hbm, aggregate_hbm, matrix, guess, right_side, restrict,
    coarse_out, residual_out,
    columns, counts, aggregate, xbuf, mbuf, wbuf, rbuf, rwbuf, rhs, part, part_in, agg_own, agg_in, con, con_in, sq, sq_in,
    load_sem, mat_sem, zsend, zrecv, xsend, xrecv, psend, precv, asend, arecv, csend, crecv, qsend, qrecv,
):
    row, col = lax.axis_index("row"), lax.axis_index("col")
    n_dev = n_row * n_col
    me = row * n_col + col
    blocks = guess.shape[0]
    own_rows = right_side.shape[0]
    slots = matrix.shape[1]
    nv = guess.shape[1]
    width = matrix.shape[3]
    r_in, r_out, _ = offsets(n_row)
    c_in, c_out, c_steps = offsets(n_col)
    z_wait = list(range(1, r_out))
    z_steps = z_wait[1:] + z_wait[:1]
    c_peers = [peer(col, c_in, c_out, s) for s in c_steps]
    z_peers = {s: row_peer(row, r_in, r_out, (s, 0)) for s in z_steps}
    x_steps = list(range(1, r_in))
    x_peers = {s: row_peer(row, r_in, r_out, (0, s)) for s in x_steps}

    own_slot = pl.ds(row * blocks, blocks)
    load_guess = pltpu.make_async_copy(guess, xbuf.at[own_slot], load_sem.at[0])
    load_guess.start()
    scalars = ((columns_hbm, columns), (counts_hbm, counts), (aggregate_hbm, aggregate))
    scalar_loads = [pltpu.make_async_copy(a, b, load_sem.at[3 + i]) for i, (a, b) in enumerate(scalars)]
    barrier = pltpu.get_barrier_semaphore()
    for p in list(z_peers.values()) + list(x_peers.values()):
        pl.semaphore_signal(barrier, inc=1, device_id=(p, col), device_id_type=pl.DeviceIdType.MESH)
    for p in c_peers:
        pl.semaphore_signal(barrier, inc=1, device_id=(row, p), device_id_type=pl.DeviceIdType.MESH)
    for c in reversed(scalar_loads):
        c.start()
    mat_loads = [pltpu.make_async_copy(matrix.at[g], mbuf.at[g], mat_sem.at[g]) for g in range(matrix.shape[0])]
    for c in mat_loads:
        c.start()
    load_restrict = pltpu.make_async_copy(restrict, rbuf, load_sem.at[1])
    load_restrict.start()
    load_rhs = pltpu.make_async_copy(right_side, rhs, load_sem.at[2])
    load_rhs.start()
    load_guess.wait()
    pl.semaphore_wait(barrier, len(z_peers) + len(x_peers) + len(c_peers))

    def remote(src, dst, ssem, rsem, r, c):
        return pltpu.make_async_remote_copy(
            src_ref=src, dst_ref=dst, send_sem=ssem, recv_sem=rsem,
            device_id=(r, c), device_id_type=pl.DeviceIdType.MESH,
        )

    sends = []
    z_copies = {}
    for s in z_steps:
        z_copies[s] = remote(xbuf.at[own_slot], xbuf.at[own_slot], zsend.at[s], zrecv.at[s], z_peers[s], col)
        z_copies[s].start()
    x_copies = []
    for s in x_steps:
        c = remote(xbuf.at[own_slot], xbuf.at[own_slot], xsend.at[s, 0], xrecv.at[s, 0], x_peers[s], col)
        c.start()
        x_copies.append(c)
    scalar_loads[2].wait()
    for i in range(own_rows):
        agg_own[i] = jnp.full((8, 128), aggregate[i], jnp.int32).astype(F32)
    a_copies = []
    for k, p in enumerate(c_peers):
        c = remote(agg_own, agg_in.at[k], asend.at[k], arecv.at[k], row, p)
        c.start()
        a_copies.append(c)

    for g in range(matrix.shape[0]):
        mat_loads[g].wait()
        for s in range(slots):
            high, low = split(mbuf[g, s].T)
            wbuf[g, s * width:(s + 1) * width, :width] = high
            wbuf[g, s * width:(s + 1) * width, width:] = low
    load_restrict.wait()
    for i in range(own_rows):
        high, low = split(rbuf[i])
        rwbuf[i, :, :high.shape[1]] = high
        rwbuf[i, :, high.shape[1]:] = low

    for s in z_wait:
        z_copies[s].wait_recv()
        source = row_peer(row, r_in, r_out, (s, 0), back=True)
        got = pl.ds(source * blocks, blocks)
        for t in x_steps:
            c = remote(xbuf.at[got], xbuf.at[got], xsend.at[t, s], xrecv.at[t, s], x_peers[t], col)
            c.start()
            x_copies.append(c)
    for c in x_copies:
        c.wait_recv()

    scalar_loads[0].wait()
    scalar_loads[1].wait()

    def product(g):
        picked = []
        for s in range(slots):
            use = jnp.where(s < counts[0, g], 1.0, 0.0).astype(F32)
            picked.append(xbuf[columns[s, g]] * use)
        return dot4(jnp.concatenate(picked, axis=1), wbuf[g])

    p_copies = []
    for k, p in enumerate(c_peers):
        for i in range(own_rows):
            part[k, i] = product(p * own_rows + i)
        c = remote(part.at[k], part_in.at[k], psend.at[k], precv.at[k], row, p)
        c.start()
        p_copies.append(c)
    load_rhs.wait()
    res = [rhs[i] - product(col * own_rows + i) for i in range(own_rows)]
    for k in reversed(range(len(c_peers))):
        p_copies[k].wait_recv()
        for i in range(own_rows):
            res[i] = res[i] - part_in[k, i]

    squares = res[0] * res[0]
    for i in range(1, own_rows):
        squares = squares + res[i] * res[i]
    eye = lax.broadcasted_iota(jnp.int32, (nv, 128), 0) == lax.broadcasted_iota(jnp.int32, (nv, 128), 1)
    by_v = jnp.sum(squares, axis=1, keepdims=True)
    own_sq = jnp.sum(jnp.where(eye, by_v, 0.0), axis=0, keepdims=True)
    sq[...] = own_sq

    def send_squares(d, carry):
        t = lax.rem(me + d, n_dev)
        remote(sq, sq_in.at[d - 1], qsend, qrecv, lax.div(t, n_col), lax.rem(t, n_col)).start()
        return carry

    lax.fori_loop(1, n_dev, send_squares, 0)

    contrib = []
    for i in range(own_rows):
        contrib.append(dot4(res[i], rwbuf[i]))
        con[i] = contrib[i]
    c_copies = []
    for k, p in enumerate(c_peers):
        c = remote(con, con_in.at[k], csend.at[k], crecv.at[k], row, p)
        c.start()
        c_copies.append(c)
    for i in range(own_rows):
        residual_out[i] = res[i]

    def spread(ids, value, total):
        shaped = value.reshape(nv // 8, 8, value.shape[1])
        return [t + jnp.where(ids == c, 1.0, 0.0)[None] * shaped for c, t in enumerate(total)]

    for i in range(own_rows):
        for c in range(NC_GRP):
            mask = jnp.where(agg_own[i] == c, 1.0, 0.0)[None]
            term = mask * contrib[i].reshape(nv // 8, 8, 128)
            if i == 0:
                coarse_out[c] = term.reshape(nv, 128)
            else:
                coarse_out[c] += term.reshape(nv, 128)
    for c in a_copies:
        c.wait_recv()
    for c in c_copies:
        c.wait_recv()
    for c in range(NC_GRP):
        total = coarse_out[c].reshape(nv // 8, 8, 128)
        for k in range(len(c_peers)):
            for i in range(own_rows):
                mask = jnp.where(agg_in[k, i] == c, 1.0, 0.0)[None]
                total = total + mask * con_in[k, i].reshape(nv // 8, 8, 128)
        coarse_out[c] = total.reshape(nv, 128)

    pltpu.make_async_copy(sq_in, sq_in, qrecv).wait()
    all_sq = own_sq + jnp.sum(sq_in[...], axis=0)
    total_v = jnp.sum(jnp.where(eye, all_sq, 0.0), axis=1, keepdims=True)
    inv = 1.0 / jnp.sqrt(total_v / (n_dev * own_rows * 128) + 1e-06)
    for c in range(NC_GRP):
        coarse_out[c] = coarse_out[c] * inv

    for c in list(z_copies.values()) + x_copies + a_copies + p_copies + c_copies:
        c.wait_send()
    pltpu.make_async_copy(sq_in, sq_in, qsend).wait()


def local(n_row, n_col, matrix, columns, counts, fine_guess, right_side, aggregate, restrict):
    blocks, nv, bs = fine_guess.shape
    rows, slots = matrix.shape[:2]
    own_rows = right_side.shape[0]
    cw = restrict.shape[2]
    nc1 = n_col - 1
    r_in, r_out, _ = offsets(n_row)
    dma = pltpu.SemaphoreType.DMA
    vmem = pl.BlockSpec(memory_space=pltpu.VMEM)
    hbm = pl.BlockSpec(memory_space=pl.ANY)
    return pl.pallas_call(
        functools.partial(kernel, n_row, n_col),
        out_shape=(
            pltpu.VMEM((NC_GRP, nv, cw), F32),
            pltpu.VMEM(right_side.shape, F32),
        ),
        in_specs=[hbm] * 7,
        out_specs=(vmem, vmem),
        scratch_shapes=[
            pltpu.SMEM((slots, rows), jnp.int32),
            pltpu.SMEM((1, rows), jnp.int32),
            pltpu.SMEM((own_rows,), jnp.int32),
            pltpu.VMEM((n_row * blocks, nv, bs), F32),
            pltpu.VMEM(matrix.shape, F32),
            pltpu.VMEM((rows, slots * bs, 2 * bs), BF16),
            pltpu.VMEM(restrict.shape, F32),
            pltpu.VMEM((own_rows, bs, 2 * cw), BF16),
            pltpu.VMEM(right_side.shape, F32),
            pltpu.VMEM((nc1, own_rows, nv, bs), F32),
            pltpu.VMEM((nc1, own_rows, nv, bs), F32),
            pltpu.VMEM((own_rows, 8, 128), F32),
            pltpu.VMEM((nc1, own_rows, 8, 128), F32),
            pltpu.VMEM((own_rows, nv, cw), F32),
            pltpu.VMEM((nc1, own_rows, nv, cw), F32),
            pltpu.VMEM((1, 128), F32),
            pltpu.VMEM((n_row * n_col - 1, 1, 128), F32),
            dma((6,)), dma((rows,)),
            dma((r_out,)), dma((r_out,)),
            dma((max(r_in, 2), r_out)), dma((max(r_in, 2), r_out)),
            dma((nc1,)), dma((nc1,)),
            dma((nc1,)), dma((nc1,)),
            dma((nc1,)), dma((nc1,)),
            dma(()), dma(()),
        ],
        compiler_params=pltpu.CompilerParams(collective_id=0, has_side_effects=True),
        name="residual_restrict",
    )(columns.T, counts.T, aggregate, matrix, fine_guess, right_side, restrict)


def solution(mesh):
    in_specs = (
        P("row", "col", None, None),
        P("row", "col"),
        P("row", "col"),
        P(("col", "row"), None, None),
        P(("row", "col"), None, None),
        P(("row", "col")),
        P(("row", "col"), None, None),
    )
    out_specs = (P("row", None, None), P(("row", "col"), None, None))
    body = functools.partial(local, mesh.shape["row"], mesh.shape["col"])
    return jax.shard_map(body, mesh=mesh, in_specs=in_specs, out_specs=out_specs, check_vma=False)
```

```python
import functools

import jax
import jax.numpy as jnp
from jax import lax
from jax.experimental import pallas as pl
from jax.experimental.pallas import tpu as pltpu
from jax.sharding import PartitionSpec as P

NC_GRP = 8
F32 = jnp.float32
BF16 = jnp.bfloat16


def offsets(count):
    inner = 2 if count % 2 == 0 else 1
    outer = count // inner
    steps = [(o, i) for o in range(outer) for i in range(inner) if (o, i) != (0, 0)]
    steps.sort(key=lambda s: -min(s[0], outer - s[0]))
    return inner, outer, steps


def peer(index, inner, outer, step):
    high = lax.rem(lax.div(index, inner) + step[0], outer)
    low = lax.rem(lax.rem(index, inner) + step[1], inner)
    return high * inner + low


def swap(index, step, count):
    out, bit = 0, 1
    while bit < count:
        out = out + lax.rem(lax.div(index, bit) + (step // bit) % 2, 2) * bit
        bit *= 2
    return out


def row_peer(row, inner, outer, step, back=False):
    low = lax.rem(lax.rem(row, inner) + step[1], inner)
    if outer & (outer - 1):
        high = lax.rem(lax.div(row, inner) + (outer - step[0] if back else step[0]), outer)
    else:
        high = swap(lax.div(row, inner), step[0], outer)
    return high * inner + low


def split(value):
    high = value.astype(BF16)
    return high, (value - high.astype(F32)).astype(BF16)


def dot4(left, right):
    m, n = left.shape[0], right.shape[1] // 2
    both = jnp.concatenate(split(left), axis=0)
    out = jnp.dot(both, right, preferred_element_type=F32)
    return out[:m, :n] + (out[:m, n:] + out[m:, :n]) + out[m:, n:]


def kernel(
    n_row, n_col, columns_hbm, counts_hbm, aggregate_hbm, matrix, guess, right_side, restrict,
    coarse_out, residual_out,
    columns, counts, aggregate, xbuf, mbuf, wbuf, rbuf, rwbuf, rhs, part, part_in, agg_own, agg_in, con, con_in, sq, sq_in,
    load_sem, mat_sem, zsend, zrecv, xsend, xrecv, psend, precv, asend, arecv, csend, crecv, qsend, qrecv,
):
    row, col = lax.axis_index("row"), lax.axis_index("col")
    n_dev = n_row * n_col
    me = row * n_col + col
    blocks = guess.shape[0]
    own_rows = right_side.shape[0]
    slots = matrix.shape[1]
    nv = guess.shape[1]
    width = matrix.shape[3]
    r_in, r_out, _ = offsets(n_row)
    c_in, c_out, c_steps = offsets(n_col)
    z_wait = list(range(1, r_out))
    z_steps = z_wait[1:] + z_wait[:1]
    c_peers = [peer(col, c_in, c_out, s) for s in c_steps]
    z_peers = {s: row_peer(row, r_in, r_out, (s, 0)) for s in z_steps}
    x_steps = list(range(1, r_in))
    x_peers = {s: row_peer(row, r_in, r_out, (0, s)) for s in x_steps}

    own_slot = pl.ds(row * blocks, blocks)
    load_guess = pltpu.make_async_copy(guess, xbuf.at[own_slot], load_sem.at[0])
    load_guess.start()
    scalars = ((columns_hbm, columns), (counts_hbm, counts), (aggregate_hbm, aggregate))
    scalar_loads = [pltpu.make_async_copy(a, b, load_sem.at[3 + i]) for i, (a, b) in enumerate(scalars)]
    barrier = pltpu.get_barrier_semaphore()
    for p in list(z_peers.values()) + list(x_peers.values()):
        pl.semaphore_signal(barrier, inc=1, device_id=(p, col), device_id_type=pl.DeviceIdType.MESH)
    for p in c_peers:
        pl.semaphore_signal(barrier, inc=1, device_id=(row, p), device_id_type=pl.DeviceIdType.MESH)
    for c in reversed(scalar_loads):
        c.start()
    mat_loads = [pltpu.make_async_copy(matrix.at[g], mbuf.at[g], mat_sem.at[g]) for g in range(matrix.shape[0])]
    for c in mat_loads:
        c.start()
    load_restrict = pltpu.make_async_copy(restrict, rbuf, load_sem.at[1])
    load_restrict.start()
    load_rhs = pltpu.make_async_copy(right_side, rhs, load_sem.at[2])
    load_rhs.start()
    load_guess.wait()
    pl.semaphore_wait(barrier, len(z_peers) + len(x_peers) + len(c_peers))

    def remote(src, dst, ssem, rsem, r, c):
        return pltpu.make_async_remote_copy(
            src_ref=src, dst_ref=dst, send_sem=ssem, recv_sem=rsem,
            device_id=(r, c), device_id_type=pl.DeviceIdType.MESH,
        )

    sends = []
    z_copies = {}
    for s in z_steps:
        z_copies[s] = remote(xbuf.at[own_slot], xbuf.at[own_slot], zsend.at[s], zrecv.at[s], z_peers[s], col)
        z_copies[s].start()
    x_copies = []
    for s in x_steps:
        c = remote(xbuf.at[own_slot], xbuf.at[own_slot], xsend.at[s, 0], xrecv.at[s, 0], x_peers[s], col)
        c.start()
        x_copies.append(c)
    scalar_loads[2].wait()
    for i in range(own_rows):
        agg_own[i] = jnp.full((8, 128), aggregate[i], jnp.int32).astype(F32)
    a_copies = []
    for k, p in enumerate(c_peers):
        c = remote(agg_own, agg_in.at[k], asend.at[k], arecv.at[k], row, p)
        c.start()
        a_copies.append(c)

    for g in range(matrix.shape[0]):
        mat_loads[g].wait()
        for s in range(slots):
            high, low = split(mbuf[g, s].T)
            wbuf[g, s * width:(s + 1) * width, :width] = high
            wbuf[g, s * width:(s + 1) * width, width:] = low
    load_restrict.wait()
    for i in range(own_rows):
        high, low = split(rbuf[i])
        rwbuf[i, :, :high.shape[1]] = high
        rwbuf[i, :, high.shape[1]:] = low

    for s in z_wait:
        z_copies[s].wait_recv()
        source = row_peer(row, r_in, r_out, (s, 0), back=True)
        got = pl.ds(source * blocks, blocks)
        for t in x_steps:
            c = remote(xbuf.at[got], xbuf.at[got], xsend.at[t, s], xrecv.at[t, s], x_peers[t], col)
            c.start()
            x_copies.append(c)
    for c in x_copies:
        c.wait_recv()

    scalar_loads[0].wait()
    scalar_loads[1].wait()

    def product(g):
        picked = []
        for s in range(slots):
            use = jnp.where(s < counts[0, g], 1.0, 0.0).astype(F32)
            picked.append(xbuf[columns[s, g]] * use)
        return dot4(jnp.concatenate(picked, axis=1), wbuf[g])

    p_copies = []
    for k, p in enumerate(c_peers):
        for i in range(own_rows):
            part[k, i] = product(p * own_rows + i)
        c = remote(part.at[k], part_in.at[k], psend.at[k], precv.at[k], row, p)
        c.start()
        p_copies.append(c)
    load_rhs.wait()
    res = [rhs[i] - product(col * own_rows + i) for i in range(own_rows)]
    for k in reversed(range(len(c_peers))):
        p_copies[k].wait_recv()
        for i in range(own_rows):
            res[i] = res[i] - part_in[k, i]

    squares = res[0] * res[0]
    for i in range(1, own_rows):
        squares = squares + res[i] * res[i]
    eye = lax.broadcasted_iota(jnp.int32, (nv, 128), 0) == lax.broadcasted_iota(jnp.int32, (nv, 128), 1)
    by_v = jnp.sum(squares, axis=1, keepdims=True)
    own_sq = jnp.sum(jnp.where(eye, by_v, 0.0), axis=0, keepdims=True)
    sq[...] = own_sq

    def send_squares(d, carry):
        t = lax.rem(me + d, n_dev)
        remote(sq, sq_in.at[d - 1], qsend, qrecv, lax.div(t, n_col), lax.rem(t, n_col)).start()
        return carry

    lax.fori_loop(1, n_dev, send_squares, 0)

    contrib = []
    for i in range(own_rows):
        contrib.append(dot4(res[i], rwbuf[i]))
        con[i] = contrib[i]
    c_copies = []
    for k, p in enumerate(c_peers):
        c = remote(con, con_in.at[k], csend.at[k], crecv.at[k], row, p)
        c.start()
        c_copies.append(c)
    for i in range(own_rows):
        residual_out[i] = res[i]

    def spread(ids, value, total):
        shaped = value.reshape(nv // 8, 8, value.shape[1])
        return [t + jnp.where(ids == c, 1.0, 0.0)[None] * shaped for c, t in enumerate(total)]

    for i in range(own_rows):
        for c in range(NC_GRP):
            mask = jnp.where(agg_own[i] == c, 1.0, 0.0)[None]
            term = mask * contrib[i].reshape(nv // 8, 8, 128)
            if i == 0:
                coarse_out[c] = term.reshape(nv, 128)
            else:
                coarse_out[c] += term.reshape(nv, 128)
    for c in a_copies:
        c.wait_recv()
    for c in c_copies:
        c.wait_recv()
    for c in range(NC_GRP):
        total = coarse_out[c].reshape(nv // 8, 8, 128)
        for k in range(len(c_peers)):
            for i in range(own_rows):
                mask = jnp.where(agg_in[k, i] == c, 1.0, 0.0)[None]
                total = total + mask * con_in[k, i].reshape(nv // 8, 8, 128)
        coarse_out[c] = total.reshape(nv, 128)

    pltpu.make_async_copy(sq_in, sq_in, qrecv).wait()
    all_sq = own_sq + jnp.sum(sq_in[...], axis=0)
    total_v = jnp.sum(jnp.where(eye, all_sq, 0.0), axis=1, keepdims=True)
    inv = 1.0 / jnp.sqrt(total_v / (n_dev * own_rows * 128) + 1e-06)
    for c in range(NC_GRP):
        coarse_out[c] = coarse_out[c] * inv

    for c in list(z_copies.values()) + x_copies + a_copies + p_copies + c_copies:
        c.wait_send()
    pltpu.make_async_copy(sq_in, sq_in, qsend).wait()


def store(coarse, residual, coarse_out, residual_out, sem):
    copies = [
        pltpu.make_async_copy(coarse, coarse_out, sem.at[0]),
        pltpu.make_async_copy(residual, residual_out, sem.at[1]),
    ]
    for c in copies:
        c.start()
    for c in copies:
        c.wait()


def local(n_row, n_col, matrix, columns, counts, fine_guess, right_side, aggregate, restrict):
    blocks, nv, bs = fine_guess.shape
    rows, slots = matrix.shape[:2]
    own_rows = right_side.shape[0]
    cw = restrict.shape[2]
    nc1 = n_col - 1
    r_in, r_out, _ = offsets(n_row)
    dma = pltpu.SemaphoreType.DMA
    vmem = pl.BlockSpec(memory_space=pltpu.VMEM)
    hbm = pl.BlockSpec(memory_space=pl.ANY)
    coarse, residual = pl.pallas_call(
        functools.partial(kernel, n_row, n_col),
        out_shape=(
            pltpu.VMEM((NC_GRP, nv, cw), F32),
            pltpu.VMEM(right_side.shape, F32),
        ),
        in_specs=[hbm] * 7,
        out_specs=(vmem, vmem),
        scratch_shapes=[
            pltpu.SMEM((slots, rows), jnp.int32),
            pltpu.SMEM((1, rows), jnp.int32),
            pltpu.SMEM((own_rows,), jnp.int32),
            pltpu.VMEM((n_row * blocks, nv, bs), F32),
            pltpu.VMEM(matrix.shape, F32),
            pltpu.VMEM((rows, slots * bs, 2 * bs), BF16),
            pltpu.VMEM(restrict.shape, F32),
            pltpu.VMEM((own_rows, bs, 2 * cw), BF16),
            pltpu.VMEM(right_side.shape, F32),
            pltpu.VMEM((nc1, own_rows, nv, bs), F32),
            pltpu.VMEM((nc1, own_rows, nv, bs), F32),
            pltpu.VMEM((own_rows, 8, 128), F32),
            pltpu.VMEM((nc1, own_rows, 8, 128), F32),
            pltpu.VMEM((own_rows, nv, cw), F32),
            pltpu.VMEM((nc1, own_rows, nv, cw), F32),
            pltpu.VMEM((1, 128), F32),
            pltpu.VMEM((n_row * n_col - 1, 1, 128), F32),
            dma((6,)), dma((rows,)),
            dma((r_out,)), dma((r_out,)),
            dma((max(r_in, 2), r_out)), dma((max(r_in, 2), r_out)),
            dma((nc1,)), dma((nc1,)),
            dma((nc1,)), dma((nc1,)),
            dma((nc1,)), dma((nc1,)),
            dma(()), dma(()),
        ],
        compiler_params=pltpu.CompilerParams(collective_id=0, has_side_effects=True),
        name="residual_restrict",
    )(columns.T, counts.T, aggregate, matrix, fine_guess, right_side, restrict)
    coarse = pltpu.with_memory_space_constraint(coarse, pltpu.VMEM)
    residual = pltpu.with_memory_space_constraint(residual, pltpu.VMEM)
    return pl.pallas_call(
        store,
        out_shape=(jax.ShapeDtypeStruct(coarse.shape, F32), jax.ShapeDtypeStruct(residual.shape, F32)),
        in_specs=[vmem, vmem],
        out_specs=(hbm, hbm),
        scratch_shapes=[dma((2,))],
        name="store",
    )(coarse, residual)


def solution(mesh):
    in_specs = (
        P("row", "col", None, None),
        P("row", "col"),
        P("row", "col"),
        P(("col", "row"), None, None),
        P(("row", "col"), None, None),
        P(("row", "col")),
        P(("row", "col"), None, None),
    )
    out_specs = (P("row", None, None), P(("row", "col"), None, None))
    body = functools.partial(local, mesh.shape["row"], mesh.shape["col"])
    return jax.shard_map(body, mesh=mesh, in_specs=in_specs, out_specs=out_specs, check_vma=False)
```

```python
import functools

import jax
import jax.numpy as jnp
from jax import lax
from jax.experimental import pallas as pl
from jax.experimental.pallas import tpu as pltpu
from jax.sharding import PartitionSpec as P

NC_GRP = 8
F32 = jnp.float32
BF16 = jnp.bfloat16


def offsets(count):
    inner = 2 if count % 2 == 0 else 1
    outer = count // inner
    steps = [(o, i) for o in range(outer) for i in range(inner) if (o, i) != (0, 0)]
    steps.sort(key=lambda s: -min(s[0], outer - s[0]))
    return inner, outer, steps


def peer(index, inner, outer, step):
    high = lax.rem(lax.div(index, inner) + step[0], outer)
    low = lax.rem(lax.rem(index, inner) + step[1], inner)
    return high * inner + low


def swap(index, step, count):
    out, bit = 0, 1
    while bit < count:
        out = out + lax.rem(lax.div(index, bit) + (step // bit) % 2, 2) * bit
        bit *= 2
    return out


def row_peer(row, inner, outer, step, back=False):
    low = lax.rem(lax.rem(row, inner) + step[1], inner)
    if outer & (outer - 1):
        high = lax.rem(lax.div(row, inner) + (outer - step[0] if back else step[0]), outer)
    else:
        high = swap(lax.div(row, inner), step[0], outer)
    return high * inner + low


def split(value):
    high = value.astype(BF16)
    return high, (value - high.astype(F32)).astype(BF16)


def dot4(left, right):
    m, n = left.shape[0], right.shape[1] // 2
    both = jnp.concatenate(split(left), axis=0)
    out = jnp.dot(both, right, preferred_element_type=F32)
    return out[:m, :n] + (out[:m, n:] + out[m:, :n]) + out[m:, n:]


def kernel(
    n_row, n_col, columns_hbm, counts_hbm, aggregate_hbm, matrix, guess, right_side, restrict,
    coarse_out, residual_out,
    columns, counts, aggregate, xbuf, mbuf, wbuf, rbuf, rwbuf, rhs, part, part_in, agg_own, agg_in, con, con_in, sq, sq_in,
    load_sem, mat_sem, zsend, zrecv, xsend, xrecv, psend, precv, asend, arecv, csend, crecv, qsend, qrecv,
):
    row, col = lax.axis_index("row"), lax.axis_index("col")
    n_dev = n_row * n_col
    me = row * n_col + col
    blocks = guess.shape[0]
    own_rows = right_side.shape[0]
    slots = matrix.shape[1]
    nv = guess.shape[1]
    width = matrix.shape[3]
    r_in, r_out, _ = offsets(n_row)
    c_in, c_out, c_steps = offsets(n_col)
    z_wait = list(range(1, r_out))
    z_steps = z_wait[1:] + z_wait[:1]
    c_peers = [peer(col, c_in, c_out, s) for s in c_steps]
    z_peers = {s: row_peer(row, r_in, r_out, (s, 0)) for s in z_steps}
    x_steps = list(range(1, r_in))
    x_peers = {s: row_peer(row, r_in, r_out, (0, s)) for s in x_steps}

    own_slot = pl.ds(row * blocks, blocks)
    load_guess = pltpu.make_async_copy(guess, xbuf.at[own_slot], load_sem.at[0])
    load_guess.start()
    scalars = ((columns_hbm, columns), (counts_hbm, counts), (aggregate_hbm, aggregate))
    scalar_loads = [pltpu.make_async_copy(a, b, load_sem.at[3 + i]) for i, (a, b) in enumerate(scalars)]
    barrier = pltpu.get_barrier_semaphore()
    for p in list(z_peers.values()) + list(x_peers.values()):
        pl.semaphore_signal(barrier, inc=1, device_id=(p, col), device_id_type=pl.DeviceIdType.MESH)
    for p in c_peers:
        pl.semaphore_signal(barrier, inc=1, device_id=(row, p), device_id_type=pl.DeviceIdType.MESH)
    load_guess.wait()
    pl.semaphore_wait(barrier, len(z_peers) + len(x_peers) + len(c_peers))

    def remote(src, dst, ssem, rsem, r, c):
        return pltpu.make_async_remote_copy(
            src_ref=src, dst_ref=dst, send_sem=ssem, recv_sem=rsem,
            device_id=(r, c), device_id_type=pl.DeviceIdType.MESH,
        )

    sends = []
    z_copies = {}
    for s in z_steps:
        z_copies[s] = remote(xbuf.at[own_slot], xbuf.at[own_slot], zsend.at[s], zrecv.at[s], z_peers[s], col)
        z_copies[s].start()
    x_copies = []
    for s in x_steps:
        c = remote(xbuf.at[own_slot], xbuf.at[own_slot], xsend.at[s, 0], xrecv.at[s, 0], x_peers[s], col)
        c.start()
        x_copies.append(c)
    for c in reversed(scalar_loads):
        c.start()
    mat_loads = [pltpu.make_async_copy(matrix.at[g], mbuf.at[g], mat_sem.at[g]) for g in range(matrix.shape[0])]
    for c in mat_loads:
        c.start()
    load_restrict = pltpu.make_async_copy(restrict, rbuf, load_sem.at[1])
    load_restrict.start()
    load_rhs = pltpu.make_async_copy(right_side, rhs, load_sem.at[2])
    load_rhs.start()
    scalar_loads[2].wait()
    for i in range(own_rows):
        agg_own[i] = jnp.full((8, 128), aggregate[i], jnp.int32).astype(F32)
    a_copies = []
    for k, p in enumerate(c_peers):
        c = remote(agg_own, agg_in.at[k], asend.at[k], arecv.at[k], row, p)
        c.start()
        a_copies.append(c)

    for g in range(matrix.shape[0]):
        mat_loads[g].wait()
        for s in range(slots):
            high, low = split(mbuf[g, s].T)
            wbuf[g, s * width:(s + 1) * width, :width] = high
            wbuf[g, s * width:(s + 1) * width, width:] = low
    load_restrict.wait()
    for i in range(own_rows):
        high, low = split(rbuf[i])
        rwbuf[i, :, :high.shape[1]] = high
        rwbuf[i, :, high.shape[1]:] = low

    for s in z_wait:
        z_copies[s].wait_recv()
        source = row_peer(row, r_in, r_out, (s, 0), back=True)
        got = pl.ds(source * blocks, blocks)
        for t in x_steps:
            c = remote(xbuf.at[got], xbuf.at[got], xsend.at[t, s], xrecv.at[t, s], x_peers[t], col)
            c.start()
            x_copies.append(c)
    for c in x_copies:
        c.wait_recv()

    scalar_loads[0].wait()
    scalar_loads[1].wait()

    def product(g):
        picked = []
        for s in range(slots):
            use = jnp.where(s < counts[0, g], 1.0, 0.0).astype(F32)
            picked.append(xbuf[columns[s, g]] * use)
        return dot4(jnp.concatenate(picked, axis=1), wbuf[g])

    p_copies = []
    for k, p in enumerate(c_peers):
        for i in range(own_rows):
            part[k, i] = product(p * own_rows + i)
        c = remote(part.at[k], part_in.at[k], psend.at[k], precv.at[k], row, p)
        c.start()
        p_copies.append(c)
    load_rhs.wait()
    res = [rhs[i] - product(col * own_rows + i) for i in range(own_rows)]
    for k in reversed(range(len(c_peers))):
        p_copies[k].wait_recv()
        for i in range(own_rows):
            res[i] = res[i] - part_in[k, i]

    squares = res[0] * res[0]
    for i in range(1, own_rows):
        squares = squares + res[i] * res[i]
    eye = lax.broadcasted_iota(jnp.int32, (nv, 128), 0) == lax.broadcasted_iota(jnp.int32, (nv, 128), 1)
    by_v = jnp.sum(squares, axis=1, keepdims=True)
    own_sq = jnp.sum(jnp.where(eye, by_v, 0.0), axis=0, keepdims=True)
    sq[...] = own_sq

    def send_squares(d, carry):
        t = lax.rem(me + d, n_dev)
        remote(sq, sq_in.at[d - 1], qsend, qrecv, lax.div(t, n_col), lax.rem(t, n_col)).start()
        return carry

    lax.fori_loop(1, n_dev, send_squares, 0)

    contrib = []
    for i in range(own_rows):
        contrib.append(dot4(res[i], rwbuf[i]))
        con[i] = contrib[i]
    c_copies = []
    for k, p in enumerate(c_peers):
        c = remote(con, con_in.at[k], csend.at[k], crecv.at[k], row, p)
        c.start()
        c_copies.append(c)
    for i in range(own_rows):
        residual_out[i] = res[i]

    def spread(ids, value, total):
        shaped = value.reshape(nv // 8, 8, value.shape[1])
        return [t + jnp.where(ids == c, 1.0, 0.0)[None] * shaped for c, t in enumerate(total)]

    for i in range(own_rows):
        for c in range(NC_GRP):
            mask = jnp.where(agg_own[i] == c, 1.0, 0.0)[None]
            term = mask * contrib[i].reshape(nv // 8, 8, 128)
            if i == 0:
                coarse_out[c] = term.reshape(nv, 128)
            else:
                coarse_out[c] += term.reshape(nv, 128)
    for c in a_copies:
        c.wait_recv()
    for k in reversed(range(len(c_peers))):
        c_copies[k].wait_recv()
        for c in range(NC_GRP):
            total = coarse_out[c].reshape(nv // 8, 8, 128)
            for i in range(own_rows):
                mask = jnp.where(agg_in[k, i] == c, 1.0, 0.0)[None]
                total = total + mask * con_in[k, i].reshape(nv // 8, 8, 128)
            coarse_out[c] = total.reshape(nv, 128)

    pltpu.make_async_copy(sq_in, sq_in, qrecv).wait()
    all_sq = own_sq + jnp.sum(sq_in[...], axis=0)
    total_v = jnp.sum(jnp.where(eye, all_sq, 0.0), axis=1, keepdims=True)
    inv = 1.0 / jnp.sqrt(total_v / (n_dev * own_rows * 128) + 1e-06)
    for c in range(NC_GRP):
        coarse_out[c] = coarse_out[c] * inv

    for c in list(z_copies.values()) + x_copies + a_copies + p_copies + c_copies:
        c.wait_send()
    pltpu.make_async_copy(sq_in, sq_in, qsend).wait()


def store(coarse, residual, coarse_out, residual_out, sem):
    copies = [
        pltpu.make_async_copy(coarse, coarse_out, sem.at[0]),
        pltpu.make_async_copy(residual, residual_out, sem.at[1]),
    ]
    for c in copies:
        c.start()
    for c in copies:
        c.wait()


def local(n_row, n_col, matrix, columns, counts, fine_guess, right_side, aggregate, restrict):
    blocks, nv, bs = fine_guess.shape
    rows, slots = matrix.shape[:2]
    own_rows = right_side.shape[0]
    cw = restrict.shape[2]
    nc1 = n_col - 1
    r_in, r_out, _ = offsets(n_row)
    dma = pltpu.SemaphoreType.DMA
    vmem = pl.BlockSpec(memory_space=pltpu.VMEM)
    hbm = pl.BlockSpec(memory_space=pl.ANY)
    coarse, residual = pl.pallas_call(
        functools.partial(kernel, n_row, n_col),
        out_shape=(
            pltpu.VMEM((NC_GRP, nv, cw), F32),
            pltpu.VMEM(right_side.shape, F32),
        ),
        in_specs=[hbm] * 7,
        out_specs=(vmem, vmem),
        scratch_shapes=[
            pltpu.SMEM((slots, rows), jnp.int32),
            pltpu.SMEM((1, rows), jnp.int32),
            pltpu.SMEM((own_rows,), jnp.int32),
            pltpu.VMEM((n_row * blocks, nv, bs), F32),
            pltpu.VMEM(matrix.shape, F32),
            pltpu.VMEM((rows, slots * bs, 2 * bs), BF16),
            pltpu.VMEM(restrict.shape, F32),
            pltpu.VMEM((own_rows, bs, 2 * cw), BF16),
            pltpu.VMEM(right_side.shape, F32),
            pltpu.VMEM((nc1, own_rows, nv, bs), F32),
            pltpu.VMEM((nc1, own_rows, nv, bs), F32),
            pltpu.VMEM((own_rows, 8, 128), F32),
            pltpu.VMEM((nc1, own_rows, 8, 128), F32),
            pltpu.VMEM((own_rows, nv, cw), F32),
            pltpu.VMEM((nc1, own_rows, nv, cw), F32),
            pltpu.VMEM((1, 128), F32),
            pltpu.VMEM((n_row * n_col - 1, 1, 128), F32),
            dma((6,)), dma((rows,)),
            dma((r_out,)), dma((r_out,)),
            dma((max(r_in, 2), r_out)), dma((max(r_in, 2), r_out)),
            dma((nc1,)), dma((nc1,)),
            dma((nc1,)), dma((nc1,)),
            dma((nc1,)), dma((nc1,)),
            dma(()), dma(()),
        ],
        compiler_params=pltpu.CompilerParams(collective_id=0, has_side_effects=True),
        name="residual_restrict",
    )(columns.T, counts.T, aggregate, matrix, fine_guess, right_side, restrict)
    coarse = pltpu.with_memory_space_constraint(coarse, pltpu.VMEM)
    residual = pltpu.with_memory_space_constraint(residual, pltpu.VMEM)
    return pl.pallas_call(
        store,
        out_shape=(jax.ShapeDtypeStruct(coarse.shape, F32), jax.ShapeDtypeStruct(residual.shape, F32)),
        in_specs=[vmem, vmem],
        out_specs=(hbm, hbm),
        scratch_shapes=[dma((2,))],
        name="store",
    )(coarse, residual)


def solution(mesh):
    in_specs = (
        P("row", "col", None, None),
        P("row", "col"),
        P("row", "col"),
        P(("col", "row"), None, None),
        P(("row", "col"), None, None),
        P(("row", "col")),
        P(("row", "col"), None, None),
    )
    out_specs = (P("row", None, None), P(("row", "col"), None, None))
    body = functools.partial(local, mesh.shape["row"], mesh.shape["col"])
    return jax.shard_map(body, mesh=mesh, in_specs=in_specs, out_specs=out_specs, check_vma=False)
```
